256 devices in a mesh: time: 64 (over z_lo, y, x, core), chan: 4 (over z_hi).
Axes of the slice: x: 4, y: 4, z: 8 (z_hi: 4, z_lo: 2; z = z_hi * 2 + z_lo), core: 2. Of those that a mesh axis runs over, the one named last changes fastest.
Arguments:
- decay_rate: float32 [4, 32768, 2560], P(None, 'time', 'chan'), may hold values from 0.2 to 2
- drive_in: bfloat16 [4, 32768, 2560], P(None, 'time', 'chan'), may hold values from -6 to 6
- gate_in: bfloat16 [4, 32768, 2560], P(None, 'time', 'chan'), may hold values from -6 to 6
- norm_gain: float32 [2560], P('chan'), may hold values from 0.25 to 1.75
Outputs:
- filtered: bfloat16 [4, 32768, 2560], P(None, 'time', 'chan')
The draws below stay inside these ranges and needn't reach their ends.
All inputs are finite; a program needn't handle non-finite values.
Results may differ from the reference program's by a relative error of at most 0.0015.
Values sent between devices are 32-bit elements.
No kernel may reach another device: no remote copies, remote signals or barrier semaphores. Data moves between devices by JAX's collectives and lax.ppermute only.
A program may use at most 128 MiB of HBM per device.

```python
import jax
import jax.numpy as jnp
from jax import lax

BATCH = 4
CHANNELS = 2560
LENGTH = 32768


def levels(rng, extent, cuts, least, largest):
    level = 1.0
    for position, shards_of in cuts:
        steps = jax.random.uniform(jax.random.fold_in(jax.random.fold_in(rng, 6), position), (shards_of,), jnp.float32, least / len(cuts), largest / len(cuts))
        level = level * jnp.repeat(jnp.exp(steps), extent[position] // shards_of).reshape((-1,) + (1,) * (len(extent) - 1 - position))
    return level


def bell_draw(key, dims, scale, limit, pieces=(), kind=jnp.bfloat16):
    array = scale * jax.random.normal(key, dims, jnp.float32)
    if pieces:
        array = array * levels(key, dims, pieces, -0.22, 0.18)
    return jnp.clip(array, -limit, limit).astype(kind)


def setup_inputs(seed: int = 0) -> dict:
    arg_keys = jax.random.split(jax.random.key(seed), 5)
    return {
        "decay_rate": jnp.clip(0.2 + 1.8 * jax.random.uniform(arg_keys[0], (BATCH, LENGTH, CHANNELS), jnp.float32) ** levels(arg_keys[0], (BATCH, LENGTH, CHANNELS), ((1, 64), (2, 4)), -0.2, 0.2), 0.2, 2.0),
        "drive_in": bell_draw(arg_keys[1], (BATCH, LENGTH, CHANNELS), 1.0, 6.0, ((1, 64), (2, 4))),
        "gate_in": bell_draw(arg_keys[2], (BATCH, LENGTH, CHANNELS), 1.0, 6.0, ((1, 64), (2, 4))),
        "norm_gain": jnp.clip(1.0 + 0.15 * jax.random.normal(arg_keys[3], (CHANNELS,), jnp.float32), 0.25, 1.75),
    }


def join_pair(earlier, later):
    return (earlier[0] * later[0], later[0] * earlier[1] + later[1])

def reference(decay_rate, drive_in, gate_in, norm_gain):
    keep = jnp.exp(-decay_rate / LENGTH)
    push = drive_in.astype(jnp.float32) * LENGTH ** (-0.5)
    forward = lax.associative_scan(join_pair, (keep, push), axis=1)[1]
    gated = forward * jax.nn.sigmoid(gate_in.astype(jnp.float32))
    power = lax.optimization_barrier(jnp.mean(gated * gated, axis=-1, keepdims=True))
    filtered = (gated * lax.rsqrt(power + 1e-06) * norm_gain).astype(jnp.bfloat16)
    return filtered
```

```python
import jax
import jax.numpy as jnp
import numpy as np
from jax import lax
from jax.experimental import pallas as pl
from jax.experimental.pallas import tpu as pltpu
from jax.sharding import Mesh
from jax.sharding import PartitionSpec as P

TIME = ("time_0", "time_1", "time_2", "time_3")
CHIPS = ("time_0", "time_1", "time_2")
CORE = "time_3"
CHUNK = 256
SWAP = [(0, 1), (1, 0)]


def later_sums(decay, later_ref):
    return jnp.dot(later_ref[...], decay.astype(jnp.bfloat16), preferred_element_type=jnp.float32)


def summary_kernel(scale, decay_ref, drive_ref, later_ref, chunk_ref, total_ref):
    j = pl.program_id(1)
    decay = decay_ref[0]
    drive = drive_ref[0].astype(jnp.float32)
    pushed = jnp.sum(jnp.exp(later_sums(decay, later_ref)) * drive, axis=0, keepdims=True)
    lost = jnp.sum(decay, axis=0, keepdims=True) * scale
    chunk_ref[0, 0, 0:1] = lost
    chunk_ref[0, 0, 1:2] = pushed

    @pl.when(j == 0)
    def _():
        total_ref[0, 0:1] = lost
        total_ref[0, 1:2] = pushed

    @pl.when(j > 0)
    def _():
        total_ref[0, 0:1] = total_ref[0, 0:1] + lost
        total_ref[0, 1:2] = jnp.exp(-lost) * total_ref[0, 1:2] + pushed


def local_kernel(decay_ref, drive_ref, gate_ref, later_ref, upto_ref, after_ref, run_ref, open_ref):
    del after_ref
    logs = later_sums(decay_ref[0], later_ref)
    weight = jnp.exp(logs)
    drive = drive_ref[0]
    less = (drive.astype(jnp.float32) * (1.0 - weight)).astype(jnp.bfloat16)
    run_ref[0] = jnp.dot(upto_ref[...], drive, preferred_element_type=jnp.float32) - jnp.dot(
        upto_ref[...], less, preferred_element_type=jnp.float32
    )
    gate = 0.5 * jnp.tanh(0.5 * gate_ref[0].astype(jnp.float32)) + 0.5
    open_ref[0] = jnp.exp(-logs) * gate


def power_kernel(run_ref, open_ref, start_ref, chunk_ref, gated_ref, power_ref, carry_ref):
    j = pl.program_id(1)

    @pl.when(j == 0)
    def _():
        carry_ref[...] = start_ref[0]

    kept = carry_ref[...] * jnp.exp(-chunk_ref[0, 0, 0:1])
    gated = (run_ref[0] + kept) * open_ref[0]
    carry_ref[...] = kept + chunk_ref[0, 0, 1:2]
    gated_ref[0] = gated
    square = gated * gated
    lanes = sum(square[:, k * 128 : (k + 1) * 128] for k in range(square.shape[1] // 128))
    power_ref[0, 0] = jnp.sum(lanes.T, axis=0, keepdims=True)


def norm_kernel(channels, eps, gated_ref, power_ref, gain_ref, out_ref):
    rate = lax.rsqrt(power_ref[0, 0] * (1.0 / channels) + eps)
    rate = jnp.broadcast_to(rate, (128, rate.shape[1])).T
    gated = gated_ref[0]
    for k in range(gated.shape[1] // 128):
        at = slice(k * 128, (k + 1) * 128)
        out_ref[0, :, at] = (gated[:, at] * rate * gain_ref[:, at]).astype(jnp.bfloat16)


def params(mib):
    return pltpu.CompilerParams(
        dimension_semantics=("arbitrary", "arbitrary"), vmem_limit_bytes=mib * 1024 * 1024
    )


def join_pair(earlier, later):
    return (earlier[0] + later[0], jnp.exp(-later[0]) * earlier[1] + later[1])


def total_over_chan(x):
    x = x + lax.ppermute(x, "chan", [(i, i ^ 1) for i in range(4)])
    return x + lax.ppermute(x, "chan", [(i, i ^ 3) for i in range(4)])


def body(decay_rate, drive_in, gate_in, norm_gain):
    batch, length, width = decay_rate.shape
    total_length = length * lax.axis_size(TIME)
    channels = width * lax.axis_size("chan")
    chunks = length // CHUNK
    half = batch // 2
    row = np.arange(CHUNK)
    later = jnp.asarray((row[None, :] > row[:, None]) * (-1.0 / total_length), jnp.bfloat16)
    upto = jnp.asarray(row[None, :] <= row[:, None], jnp.bfloat16)
    grid = (batch, chunks)
    block = pl.BlockSpec((1, CHUNK, width), lambda b, j: (b, j, 0))
    square = pl.BlockSpec((CHUNK, CHUNK), lambda b, j: (0, 0))
    by_chunk = pl.BlockSpec((1, 1, 2, width), lambda b, j: (b, j, 0, 0))
    by_batch = pl.BlockSpec((1, 2, width), lambda b, j: (b, 0, 0))
    f32 = jnp.float32
    wide = jax.ShapeDtypeStruct((batch, length, width), f32)

    chunk, total = pl.pallas_call(
        lambda *refs: summary_kernel(1.0 / total_length, *refs),
        grid=grid,
        in_specs=[block, block, square],
        out_specs=[by_chunk, by_batch],
        out_shape=[
            jax.ShapeDtypeStruct((batch, chunks, 2, width), f32),
            jax.ShapeDtypeStruct((batch, 2, width), f32),
        ],
        compiler_params=params(12),
        name="summary",
    )(decay_rate, drive_in, later)

    core, chip = lax.axis_index(CORE), lax.axis_index(CHIPS)
    other = lax.ppermute(total, CORE, SWAP)
    first = jnp.where(core == 0, total, other)
    second = jnp.where(core == 0, other, total)
    lost, pushed = join_pair((first[:, 0], first[:, 1]), (second[:, 0], second[:, 1]))
    both = jnp.stack([lost, pushed])
    both = jnp.where(core == 0, both[:, :half], both[:, half:])
    peers = lax.axis_size(CHIPS)
    sent = jnp.broadcast_to(both, (peers,) + both.shape)
    pieces = lax.all_to_all(sent, CHIPS, 0, 0)

    run, opened = pl.pallas_call(
        local_kernel,
        grid=grid,
        in_specs=[block, block, block, square, square, pl.BlockSpec((1, 2, width), lambda b, j: (0, 0, 0))],
        out_specs=[block, block],
        out_shape=[wide, wide],
        compiler_params=params(16),
        cost_estimate=pl.CostEstimate(flops=4_000_000_000, transcendentals=0, bytes_accessed=20_000_000),
        name="local",
    )(decay_rate, drive_in, gate_in, later, upto, both)

    carry = jnp.zeros_like(both[0])
    for k in range(peers - 1):
        carry = jnp.where(k < chip, jnp.exp(-pieces[k, 0]) * carry + pieces[k, 1], carry)
    across = lax.ppermute(carry, CORE, SWAP)
    carry = jnp.where(
        core == 0, jnp.concatenate([carry, across]), jnp.concatenate([across, carry])
    )
    start = jnp.where(core == 0, carry, jnp.exp(-first[:, 0]) * carry + first[:, 1])

    gated, power = pl.pallas_call(
        power_kernel,
        grid=grid,
        in_specs=[block, block, pl.BlockSpec((1, 1, width), lambda b, j: (b, 0, 0)), by_chunk],
        out_specs=[block, pl.BlockSpec((1, 1, 1, CHUNK), lambda b, j: (b, j, 0, 0))],
        out_shape=[wide, jax.ShapeDtypeStruct((batch, chunks, 1, CHUNK), f32)],
        scratch_shapes=[pltpu.VMEM((1, width), f32)],
        compiler_params=params(12),
        name="power",
    )(run, opened, start[:, None], chunk)

    power = total_over_chan(power)

    return pl.pallas_call(
        lambda *refs: norm_kernel(channels, 1e-6 * total_length, *refs),
        grid=grid,
        in_specs=[
            block,
            pl.BlockSpec((1, 1, 1, CHUNK), lambda b, j: (b, j, 0, 0)),
            pl.BlockSpec((1, width), lambda b, j: (0, 0)),
        ],
        out_specs=block,
        out_shape=jax.ShapeDtypeStruct((batch, length, width), jnp.bfloat16),
        compiler_params=params(12),
        name="norm",
    )(gated, power, norm_gain[None])


def solution(mesh):
    split = Mesh(
        mesh.devices.reshape(2, 4, 4, 2, mesh.shape["chan"]),
        TIME + ("chan",),
    )
    in_specs = (P(None, TIME, "chan"), P(None, TIME, "chan"), P(None, TIME, "chan"), P("chan"))
    out_specs = P(None, TIME, "chan")
    return jax.shard_map(body, mesh=split, in_specs=in_specs, out_specs=out_specs, check_vma=False)
```

```python
import jax
import jax.numpy as jnp
from jax import lax
from jax.experimental import pallas as pl
from jax.experimental.pallas import tpu as pltpu
from jax.sharding import Mesh
from jax.sharding import PartitionSpec as P

TIME = ("time_0", "time_1", "time_2", "time_3")
CHIPS = ("time_0", "time_1", "time_2")
CORE = "time_3"
CHUNK = 256
SWAP = [(0, 1), (1, 0)]
VMEM_LOCAL, VMEM_POWER, VMEM_NORM = 24, 8, 8


def columns(width):
    return [slice(k, min(k + 256, width)) for k in range(0, width, 256)]


def local_kernel(
    scale, place_ref, decay_hbm, drive_hbm, gate_hbm, chunk_ref, total_ref, run_ref, open_ref,
    decay_ref, drive_ref, gate_ref, later_ref, upto_ref, sems,
):
    del place_ref
    batch, length, width = decay_ref.shape
    chunks = length // CHUNK

    def loads(b, j):
        at = pl.ds(j * CHUNK, CHUNK)
        pairs = ((decay_hbm, decay_ref), (drive_hbm, drive_ref), (gate_hbm, gate_ref))
        return [
            pltpu.make_async_copy(hbm.at[b, at], ref.at[b, at], sems.at[k, b, j])
            for k, (hbm, ref) in enumerate(pairs)
        ]

    for b in range(batch):
        for j in range(chunks):
            for copy in loads(b, j):
                copy.start()

    row = lax.broadcasted_iota(jnp.int32, (CHUNK, CHUNK), 0)
    col = lax.broadcasted_iota(jnp.int32, (CHUNK, CHUNK), 1)
    later_ref[...] = jnp.where(col > row, -scale, 0.0).astype(jnp.bfloat16)
    upto_ref[...] = jnp.where(col > row, 0.0, 1.0).astype(jnp.bfloat16)
    f32 = jnp.float32

    @pl.loop(0, batch)
    def _(b):
        for j in range(chunks):
            for copy in loads(b, j):
                copy.wait()
            at = slice(j * CHUNK, (j + 1) * CHUNK)
            for cols in columns(width):
                decay = decay_ref[b, at, cols]
                drive = drive_ref[b, at, cols]
                wide = drive.astype(f32)
                logs = jnp.dot(later_ref[...], decay.astype(jnp.bfloat16), preferred_element_type=f32)
                weight = jnp.exp(logs)
                pushed = weight * wide
                less = (wide - pushed).astype(jnp.bfloat16)
                run_ref[b, at, cols] = jnp.dot(
                    upto_ref[...], drive, preferred_element_type=f32
                ) - jnp.dot(upto_ref[...], less, preferred_element_type=f32)
                gate = 0.5 * jnp.tanh(0.5 * gate_ref[b, at, cols].astype(f32)) + 0.5
                open_ref[b, at, cols] = jnp.exp(-logs) * gate
                pushed = jnp.sum(pushed, axis=0, keepdims=True)
                lost = jnp.sum(decay, axis=0, keepdims=True) * scale
                chunk_ref[b, j, 0:1, cols] = lost
                chunk_ref[b, j, 1:2, cols] = pushed
                if j == 0:
                    total_ref[b, 0:1, cols] = lost
                    total_ref[b, 1:2, cols] = pushed
                else:
                    total_ref[b, 0:1, cols] = total_ref[b, 0:1, cols] + lost
                    total_ref[b, 1:2, cols] = jnp.exp(-lost) * total_ref[b, 1:2, cols] + pushed


def pack_kernel(place_ref, total_ref, other_ref, sent_ref):
    core = place_ref[0] % 2
    batch = total_ref.shape[0]

    def half(begin, first_ref, second_ref):
        for b in range(batch // 2):
            at = begin + b
            lost = second_ref[at, 0:1]
            pushed = jnp.exp(-lost) * first_ref[at, 1:2] + second_ref[at, 1:2]
            lost = lost + first_ref[at, 0:1]
            for k in range(sent_ref.shape[0]):
                sent_ref[k, 0, b : b + 1] = lost
                sent_ref[k, 1, b : b + 1] = pushed

    @pl.when(core == 0)
    def _():
        half(0, total_ref, other_ref)

    @pl.when(core == 1)
    def _():
        half(batch // 2, other_ref, total_ref)


def carry_kernel(place_ref, pieces_ref, carry_ref):
    chip = place_ref[0] // 2
    carry = jnp.zeros(carry_ref.shape, jnp.float32)
    for k in range(pieces_ref.shape[0] - 1):
        passed = jnp.exp(-pieces_ref[k, 0]) * carry + pieces_ref[k, 1]
        carry = jnp.where(k < chip, passed, carry)
    carry_ref[...] = carry


def power_kernel(
    place_ref, run_ref, open_ref, chunk_ref, mine_ref, across_ref, other_ref,
    gated_ref, power_ref, start_ref,
):
    batch, length, width = run_ref.shape
    core = place_ref[0] % 2
    for b in range(batch):
        h, at = divmod(b, batch // 2)
        carry = jnp.where(core == h, mine_ref[at : at + 1], across_ref[at : at + 1])
        passed = jnp.exp(-other_ref[b, 0:1]) * carry + other_ref[b, 1:2]
        start_ref[b] = jnp.where(core == 0, carry, passed)

    @pl.loop(0, batch)
    def _(b):
        carry = start_ref[b]
        for j in range(length // CHUNK):
            at = slice(j * CHUNK, (j + 1) * CHUNK)
            kept = carry * jnp.exp(-chunk_ref[b, j, 0:1])
            carry = kept + chunk_ref[b, j, 1:2]
            lanes = jnp.zeros((CHUNK, 128), jnp.float32)
            for k in range(width // 128):
                cols = slice(k * 128, (k + 1) * 128)
                gated = (run_ref[b, at, cols] + kept[:, cols]) * open_ref[b, at, cols]
                gated_ref[b, at, cols] = gated
                lanes = lanes + gated * gated
            power_ref[b, j] = jnp.sum(lanes.T, axis=0, keepdims=True)


def norm_kernel(channels, eps, gated_ref, power_ref, gain_ref, out_hbm, out_ref, sems):
    batch, length, width = gated_ref.shape
    chunks = length // CHUNK

    def store(b, j):
        at = pl.ds(j * CHUNK, CHUNK)
        return pltpu.make_async_copy(out_ref.at[b, at], out_hbm.at[b, at], sems.at[b, j])

    @pl.loop(0, batch)
    def _(b):
        for j in range(chunks):
            at = slice(j * CHUNK, (j + 1) * CHUNK)
            rate = lax.rsqrt(power_ref[b, j] * (1.0 / channels) + eps)
            rate = jnp.broadcast_to(rate, (128, CHUNK)).T
            for k in range(width // 128):
                cols = slice(k * 128, (k + 1) * 128)
                out = gated_ref[b, at, cols] * rate * gain_ref[:, cols]
                out_ref[b, at, cols] = out.astype(jnp.bfloat16)
            store(b, j).start()

    for b in range(batch):
        for j in range(chunks):
            store(b, j).wait()


def params(mib):
    return pltpu.CompilerParams(vmem_limit_bytes=mib * 1024 * 1024)


def total_over_chan(x):
    x = x + lax.ppermute(x, "chan", [(i, i ^ 1) for i in range(4)])
    return x + lax.ppermute(x, "chan", [(i, i ^ 3) for i in range(4)])


def body(decay_rate, drive_in, gate_in, norm_gain):
    batch, length, width = decay_rate.shape
    total_length = length * lax.axis_size(TIME)
    channels = width * lax.axis_size("chan")
    chunks = length // CHUNK
    f32 = jnp.float32
    shape = (batch, length, width)
    hbm = pl.BlockSpec(memory_space=pltpu.HBM)
    vmem = pl.BlockSpec(memory_space=pltpu.VMEM)

    place = lax.axis_index(TIME).astype(jnp.int32).reshape(1)
    smem = pl.BlockSpec(memory_space=pltpu.SMEM)

    chunk, total, run, opened = pl.pallas_call(
        lambda *refs: local_kernel(1.0 / total_length, *refs),
        in_specs=[smem, hbm, hbm, hbm],
        out_specs=[vmem] * 4,
        out_shape=[
            jax.ShapeDtypeStruct((batch, chunks, 2, width), f32),
            jax.ShapeDtypeStruct((batch, 2, width), f32),
            jax.ShapeDtypeStruct(shape, f32),
            jax.ShapeDtypeStruct(shape, f32),
        ],
        scratch_shapes=[
            pltpu.VMEM(shape, f32),
            pltpu.VMEM(shape, jnp.bfloat16),
            pltpu.VMEM(shape, jnp.bfloat16),
            pltpu.VMEM((CHUNK, CHUNK), jnp.bfloat16),
            pltpu.VMEM((CHUNK, CHUNK), jnp.bfloat16),
            pltpu.SemaphoreType.DMA((3, batch, chunks)),
        ],
        compiler_params=params(VMEM_LOCAL),
        name="local",
    )(place, *(pltpu.with_memory_space_constraint(x, pltpu.HBM) for x in (decay_rate, drive_in, gate_in)))

    peers = lax.axis_size(CHIPS)
    other = lax.ppermute(total, CORE, SWAP)
    sent = pl.pallas_call(
        pack_kernel,
        in_specs=[smem, vmem, vmem],
        out_specs=vmem,
        out_shape=jax.ShapeDtypeStruct((peers, 2, batch // 2, width), f32),
        compiler_params=params(4),
        name="pack",
    )(place, total, other)
    pieces = lax.all_to_all(sent, CHIPS, 0, 0)
    carry = pl.pallas_call(
        carry_kernel,
        in_specs=[smem, vmem],
        out_specs=vmem,
        out_shape=jax.ShapeDtypeStruct((batch // 2, width), f32),
        compiler_params=params(4),
        name="carry",
    )(place, pieces)
    across = lax.ppermute(carry, CORE, SWAP)

    gated, power = pl.pallas_call(
        power_kernel,
        in_specs=[smem] + [vmem] * 6,
        out_specs=[vmem] * 2,
        out_shape=[
            jax.ShapeDtypeStruct(shape, f32),
            jax.ShapeDtypeStruct((batch, chunks, 1, CHUNK), f32),
        ],
        scratch_shapes=[pltpu.VMEM((batch, 1, width), f32)],
        compiler_params=params(VMEM_POWER),
        name="power",
    )(place, run, opened, chunk, carry, across, other)

    power = total_over_chan(power)

    return pl.pallas_call(
        lambda *refs: norm_kernel(channels, 1e-6 * total_length, *refs),
        in_specs=[vmem] * 3,
        out_specs=hbm,
        out_shape=jax.ShapeDtypeStruct(shape, jnp.bfloat16),
        scratch_shapes=[pltpu.VMEM(shape, jnp.bfloat16), pltpu.SemaphoreType.DMA((batch, chunks))],
        compiler_params=params(VMEM_NORM),
        name="norm",
    )(gated, power, norm_gain[None])


def solution(mesh):
    split = Mesh(
        mesh.devices.reshape(2, 4, 4, 2, mesh.shape["chan"]),
        TIME + ("chan",),
    )
    in_specs = (P(None, TIME, "chan"), P(None, TIME, "chan"), P(None, TIME, "chan"), P("chan"))
    out_specs = P(None, TIME, "chan")
    return jax.shard_map(body, mesh=split, in_specs=in_specs, out_specs=out_specs, check_vma=False)
```

```python
import jax
import jax.numpy as jnp
from jax import lax
from jax.experimental import pallas as pl
from jax.experimental.pallas import tpu as pltpu
from jax.sharding import Mesh
from jax.sharding import PartitionSpec as P

TIME = ("time_0", "time_1", "time_2", "time_3")
CHIPS = ("time_0", "time_1", "time_2")
CORE = "time_3"
CHUNK = 128
LOG2E = 1.4426950408889634
SWAP = [(0, 1), (1, 0)]
VMEM_LOCAL, VMEM_POWER, VMEM_NORM = 24, 8, 8


def columns(width):
    return [slice(k, min(k + 256, width)) for k in range(0, width, 256)]


def local_kernel(
    scale, place_ref, decay_hbm, drive_hbm, gate_hbm, chunk_ref, total_ref, run_ref, open_ref,
    decay_ref, drive_ref, gate_ref, later_ref, upto_ref, sems,
):
    del place_ref
    batch, length, width = decay_ref.shape
    chunks = length // CHUNK

    def loads(b, j):
        at = pl.ds(j * CHUNK, CHUNK)
        pairs = ((decay_hbm, decay_ref), (drive_hbm, drive_ref), (gate_hbm, gate_ref))
        return [
            pltpu.make_async_copy(hbm.at[b, at], ref.at[b, at], sems.at[k, b, j])
            for k, (hbm, ref) in enumerate(pairs)
        ]

    for j in range(chunks):
        for copy in loads(0, j):
            copy.start()

    row = lax.broadcasted_iota(jnp.int32, (CHUNK, CHUNK), 0)
    col = lax.broadcasted_iota(jnp.int32, (CHUNK, CHUNK), 1)
    bf16, f32 = jnp.bfloat16, jnp.float32
    later_ref[...] = jnp.where(col > row, -scale, 0.0).astype(bf16)
    upto = jnp.where(col > row, 0.0, 1.0).astype(bf16)
    upto_ref[:, :CHUNK] = upto
    upto_ref[:, CHUNK:] = upto

    def chunk(b, j):
        at = slice(j * CHUNK, (j + 1) * CHUNK)
        for cols in columns(width):
            decay = decay_ref[b, at, cols]
            drive = drive_ref[b, at, cols]
            logs = jnp.dot(later_ref[...], decay.astype(bf16), preferred_element_type=f32)
            less = (jnp.exp2(logs * LOG2E) - 1.0).astype(bf16) * drive
            run = jnp.dot(
                upto_ref[...], jnp.concatenate([drive, less]), preferred_element_type=f32
            )
            run_ref[b, at, cols] = run
            gate = jnp.tanh((gate_ref[b, at, cols] * bf16(0.5)).astype(f32)) + 1.0
            open_ref[b, at, cols] = jnp.exp2(logs * -LOG2E) * gate
            pushed = run[CHUNK - 1 :]
            lost = jnp.sum(decay, axis=0, keepdims=True) * scale
            chunk_ref[b, j, 0:1, cols] = lost
            chunk_ref[b, j, 1:2, cols] = pushed
            if j == 0:
                total_ref[b, 0:1, cols] = lost
                total_ref[b, 1:2, cols] = pushed
            else:
                total_ref[b, 0:1, cols] = total_ref[b, 0:1, cols] + lost
                total_ref[b, 1:2, cols] = jnp.exp(-lost) * total_ref[b, 1:2, cols] + pushed

    for j in range(chunks):
        for copy in loads(1, j):
            copy.start()
    for j in range(chunks):
        for copy in loads(0, j):
            copy.wait()
        for copy in loads(2, j):
            copy.start()
        chunk(0, j)

    @pl.loop(1, batch)
    def _(b):
        for j in range(chunks):
            for copy in loads(b, j):
                copy.wait()

        @pl.when(b < batch - 2)
        def _():
            for j in range(chunks):
                for copy in loads(b + 2, j):
                    copy.start()

        for j in range(chunks):
            chunk(b, j)


def pack_kernel(place_ref, total_ref, other_ref, sent_ref):
    core = place_ref[0] % 2
    batch = total_ref.shape[0]

    def half(begin, first_ref, second_ref):
        for b in range(batch // 2):
            at = begin + b
            lost = second_ref[at, 0:1]
            pushed = jnp.exp(-lost) * first_ref[at, 1:2] + second_ref[at, 1:2]
            lost = lost + first_ref[at, 0:1]
            for k in range(sent_ref.shape[0]):
                sent_ref[k, 0, b : b + 1] = lost
                sent_ref[k, 1, b : b + 1] = pushed

    @pl.when(core == 0)
    def _():
        half(0, total_ref, other_ref)

    @pl.when(core == 1)
    def _():
        half(batch // 2, other_ref, total_ref)


def carry_kernel(place_ref, pieces_ref, carry_ref):
    chip = place_ref[0] // 2
    carry = jnp.zeros(carry_ref.shape, jnp.float32)
    for k in range(pieces_ref.shape[0] - 1):
        passed = jnp.exp(-pieces_ref[k, 0]) * carry + pieces_ref[k, 1]
        carry = jnp.where(k < chip, passed, carry)
    carry_ref[...] = carry


def power_kernel(
    place_ref, run_ref, open_ref, chunk_ref, mine_ref, across_ref, other_ref,
    gated_ref, power_ref, start_ref,
):
    batch, length, width = run_ref.shape
    core = place_ref[0] % 2
    for b in range(batch):
        h, at = divmod(b, batch // 2)
        carry = jnp.where(core == h, mine_ref[at : at + 1], across_ref[at : at + 1])
        passed = jnp.exp(-other_ref[b, 0:1]) * carry + other_ref[b, 1:2]
        start_ref[b] = jnp.where(core == 0, carry, passed)

    @pl.loop(0, batch)
    def _(b):
        carry = start_ref[b]
        for j in range(length // CHUNK):
            at = slice(j * CHUNK, (j + 1) * CHUNK)
            kept = carry * jnp.exp(-chunk_ref[b, j, 0:1])
            carry = kept + chunk_ref[b, j, 1:2]
            lanes = jnp.zeros((CHUNK, 128), jnp.float32)
            for k in range(width // 128):
                cols = slice(k * 128, (k + 1) * 128)
                gated = (run_ref[b, at, cols] + kept[:, cols]) * open_ref[b, at, cols]
                gated_ref[b, at, cols] = gated
                lanes = lanes + gated * gated
            power_ref[b, j] = jnp.sum(lanes.T, axis=0, keepdims=True)


def norm_kernel(channels, eps, gated_ref, power_ref, gain_ref, out_hbm, out_ref, sems):
    batch, length, width = gated_ref.shape
    chunks = length // CHUNK

    def store(b, j):
        at = pl.ds(j * CHUNK, CHUNK)
        return pltpu.make_async_copy(out_ref.at[b, at], out_hbm.at[b, at], sems.at[b, j])

    @pl.loop(0, batch)
    def _(b):
        for j in range(chunks):
            at = slice(j * CHUNK, (j + 1) * CHUNK)
            rate = lax.rsqrt(power_ref[b, j] * (1.0 / channels) + eps)
            rate = jnp.broadcast_to(rate, (128, CHUNK)).T
            for k in range(width // 128):
                cols = slice(k * 128, (k + 1) * 128)
                out = gated_ref[b, at, cols] * rate * gain_ref[:, cols]
                out_ref[b, at, cols] = out.astype(jnp.bfloat16)
            store(b, j).start()

    for b in range(batch):
        for j in range(chunks):
            store(b, j).wait()


def params(mib):
    return pltpu.CompilerParams(vmem_limit_bytes=mib * 1024 * 1024)


def total_over_chan(x):
    x = x + lax.ppermute(x, "chan", [(i, i ^ 1) for i in range(4)])
    return x + lax.ppermute(x, "chan", [(i, i ^ 3) for i in range(4)])


def body(decay_rate, drive_in, gate_in, norm_gain):
    batch, length, width = decay_rate.shape
    total_length = length * lax.axis_size(TIME)
    channels = width * lax.axis_size("chan")
    chunks = length // CHUNK
    f32 = jnp.float32
    shape = (batch, length, width)
    hbm = pl.BlockSpec(memory_space=pltpu.HBM)
    vmem = pl.BlockSpec(memory_space=pltpu.VMEM)

    place = lax.axis_index(TIME).astype(jnp.int32).reshape(1)
    smem = pl.BlockSpec(memory_space=pltpu.SMEM)

    chunk, total, run, opened = pl.pallas_call(
        lambda *refs: local_kernel(1.0 / total_length, *refs),
        in_specs=[smem, hbm, hbm, hbm],
        out_specs=[vmem] * 4,
        out_shape=[
            jax.ShapeDtypeStruct((batch, chunks, 2, width), f32),
            jax.ShapeDtypeStruct((batch, 2, width), f32),
            jax.ShapeDtypeStruct(shape, f32),
            jax.ShapeDtypeStruct(shape, f32),
        ],
        scratch_shapes=[
            pltpu.VMEM(shape, f32),
            pltpu.VMEM(shape, jnp.bfloat16),
            pltpu.VMEM(shape, jnp.bfloat16),
            pltpu.VMEM((CHUNK, CHUNK), jnp.bfloat16),
            pltpu.VMEM((CHUNK, 2 * CHUNK), jnp.bfloat16),
            pltpu.SemaphoreType.DMA((3, batch, chunks)),
        ],
        compiler_params=params(VMEM_LOCAL),
        name="local",
    )(place, *(pltpu.with_memory_space_constraint(x, pltpu.HBM) for x in (decay_rate, drive_in, gate_in)))

    peers = lax.axis_size(CHIPS)
    other = lax.ppermute(total, CORE, SWAP)
    sent = pl.pallas_call(
        pack_kernel,
        in_specs=[smem, vmem, vmem],
        out_specs=vmem,
        out_shape=jax.ShapeDtypeStruct((peers, 2, batch // 2, width), f32),
        compiler_params=params(4),
        name="pack",
    )(place, total, other)
    pieces = lax.all_to_all(sent, CHIPS, 0, 0)
    carry = pl.pallas_call(
        carry_kernel,
        in_specs=[smem, vmem],
        out_specs=vmem,
        out_shape=jax.ShapeDtypeStruct((batch // 2, width), f32),
        compiler_params=params(4),
        name="carry",
    )(place, pieces)
    across = lax.ppermute(carry, CORE, SWAP)

    gated, power = pl.pallas_call(
        power_kernel,
        in_specs=[smem] + [vmem] * 6,
        out_specs=[vmem] * 2,
        out_shape=[
            jax.ShapeDtypeStruct(shape, f32),
            jax.ShapeDtypeStruct((batch, chunks, 1, CHUNK), f32),
        ],
        scratch_shapes=[pltpu.VMEM((batch, 1, width), f32)],
        compiler_params=params(VMEM_POWER),
        name="power",
    )(place, run, opened, chunk, carry, across, other)

    power = total_over_chan(power)

    return pl.pallas_call(
        lambda *refs: norm_kernel(channels, 4e-6 * total_length, *refs),
        in_specs=[vmem] * 3,
        out_specs=hbm,
        out_shape=jax.ShapeDtypeStruct(shape, jnp.bfloat16),
        scratch_shapes=[pltpu.VMEM(shape, jnp.bfloat16), pltpu.SemaphoreType.DMA((batch, chunks))],
        compiler_params=params(VMEM_NORM),
        name="norm",
    )(gated, power, norm_gain[None])


def solution(mesh):
    split = Mesh(
        mesh.devices.reshape(2, 4, 4, 2, mesh.shape["chan"]),
        TIME + ("chan",),
    )
    in_specs = (P(None, TIME, "chan"), P(None, TIME, "chan"), P(None, TIME, "chan"), P("chan"))
    out_specs = P(None, TIME, "chan")
    return jax.shard_map(body, mesh=split, in_specs=in_specs, out_specs=out_specs, check_vma=False)
```

```python
import jax
import jax.numpy as jnp
from jax import lax
from jax.experimental import pallas as pl
from jax.experimental.pallas import tpu as pltpu
from jax.sharding import Mesh
from jax.sharding import PartitionSpec as P

TIME = ("time_0", "time_1", "time_2", "time_3")
CHIPS = ("time_0", "time_1", "time_2")
CORE = "time_3"
CHUNK = 128
LOG2E = 1.4426950408889634
SWAP = [(0, 1), (1, 0)]
VMEM_LOCAL, VMEM_POWER, VMEM_NORM = 24, 8, 8


def columns(width):
    return [slice(k, min(k + 256, width)) for k in range(0, width, 256)]


def local_kernel(
    scale, place_ref, decay_hbm, drive_hbm, gate_hbm, chunk_ref, total_ref, run_ref, logs_ref,
    gate_ref, decay_ref, drive_ref, later_ref, upto_ref, sems, gate_sem,
):
    del place_ref
    batch, length, width = decay_ref.shape
    chunks = length // CHUNK

    def loads(b, j):
        at = pl.ds(j * CHUNK, CHUNK)
        pairs = ((decay_hbm, decay_ref), (drive_hbm, drive_ref))
        return [
            pltpu.make_async_copy(hbm.at[b, at], ref.at[b, at], sems.at[k, b, j])
            for k, (hbm, ref) in enumerate(pairs)
        ]

    for j in range(chunks):
        for copy in loads(0, j):
            copy.start()

    row = lax.broadcasted_iota(jnp.int32, (CHUNK, CHUNK), 0)
    col = lax.broadcasted_iota(jnp.int32, (CHUNK, CHUNK), 1)
    bf16, f32 = jnp.bfloat16, jnp.float32
    later_ref[...] = jnp.where(col > row, -scale, 0.0).astype(bf16)
    upto = jnp.where(col > row, 0.0, 1.0).astype(bf16)
    upto_ref[:, :CHUNK] = upto
    upto_ref[:, CHUNK:] = upto

    def chunk(b, j):
        at = slice(j * CHUNK, (j + 1) * CHUNK)
        for cols in columns(width):
            decay = decay_ref[b, at, cols]
            drive = drive_ref[b, at, cols]
            logs = jnp.dot(later_ref[...], decay.astype(bf16), preferred_element_type=f32)
            less = (jnp.exp2(logs * LOG2E) - 1.0).astype(bf16) * drive
            run = jnp.dot(
                upto_ref[...], jnp.concatenate([drive, less]), preferred_element_type=f32
            )
            run_ref[b, at, cols] = run
            logs_ref[b, at, cols] = logs
            pushed = run[CHUNK - 1 :]
            lost = jnp.sum(decay, axis=0, keepdims=True) * scale
            chunk_ref[b, j, 0:1, cols] = lost
            chunk_ref[b, j, 1:2, cols] = pushed
            if j == 0:
                total_ref[b, 0:1, cols] = lost
                total_ref[b, 1:2, cols] = pushed
            else:
                total_ref[b, 0:1, cols] = total_ref[b, 0:1, cols] + lost
                total_ref[b, 1:2, cols] = jnp.exp(-lost) * total_ref[b, 1:2, cols] + pushed

    gates = pltpu.make_async_copy(gate_hbm, gate_ref, gate_sem)
    for j in range(chunks):
        for copy in loads(1, j):
            copy.start()
    for j in range(chunks):
        for copy in loads(0, j):
            copy.wait()
        for copy in loads(2, j):
            copy.start()
        chunk(0, j)

    @pl.loop(1, batch)
    def _(b):
        for j in range(chunks):
            for copy in loads(b, j):
                copy.wait()

        @pl.when(b < batch - 2)
        def _():
            for j in range(chunks):
                for copy in loads(b + 2, j):
                    copy.start()

        @pl.when(b == 1)
        def _():
            gates.start()

        for j in range(chunks):
            chunk(b, j)

    gates.wait()


def gate_kernel(gate_ref, twice_ref):
    batch, length, width = gate_ref.shape

    @pl.loop(0, batch)
    def _(b):
        for j in range(length // CHUNK):
            at = slice(j * CHUNK, (j + 1) * CHUNK)
            for cols in columns(width):
                half = (gate_ref[b, at, cols] * jnp.bfloat16(0.5)).astype(jnp.float32)
                twice_ref[b, at, cols] = jnp.tanh(half) + 1.0


def open_kernel(after_ref, logs_ref, twice_ref, open_ref):
    del after_ref
    batch, length, width = logs_ref.shape

    @pl.loop(0, batch)
    def _(b):
        for j in range(length // CHUNK):
            at = slice(j * CHUNK, (j + 1) * CHUNK)
            for cols in columns(width):
                lift = jnp.exp2(logs_ref[b, at, cols] * -LOG2E)
                open_ref[b, at, cols] = lift * twice_ref[b, at, cols]


def pack_kernel(place_ref, total_ref, other_ref, after_ref, sent_ref):
    del after_ref
    core = place_ref[0] % 2
    batch = total_ref.shape[0]

    def half(begin, first_ref, second_ref):
        for b in range(batch // 2):
            at = begin + b
            lost = second_ref[at, 0:1]
            pushed = jnp.exp(-lost) * first_ref[at, 1:2] + second_ref[at, 1:2]
            lost = lost + first_ref[at, 0:1]
            for k in range(sent_ref.shape[0]):
                sent_ref[k, 0, b : b + 1] = lost
                sent_ref[k, 1, b : b + 1] = pushed

    @pl.when(core == 0)
    def _():
        half(0, total_ref, other_ref)

    @pl.when(core == 1)
    def _():
        half(batch // 2, other_ref, total_ref)


def carry_kernel(place_ref, pieces_ref, carry_ref):
    chip = place_ref[0] // 2
    carry = jnp.zeros(carry_ref.shape, jnp.float32)
    for k in range(pieces_ref.shape[0] - 1):
        passed = jnp.exp(-pieces_ref[k, 0]) * carry + pieces_ref[k, 1]
        carry = jnp.where(k < chip, passed, carry)
    carry_ref[...] = carry


def power_kernel(
    place_ref, run_ref, open_ref, chunk_ref, mine_ref, across_ref, other_ref,
    gated_ref, power_ref, start_ref,
):
    batch, length, width = run_ref.shape
    core = place_ref[0] % 2
    for b in range(batch):
        h, at = divmod(b, batch // 2)
        carry = jnp.where(core == h, mine_ref[at : at + 1], across_ref[at : at + 1])
        passed = jnp.exp(-other_ref[b, 0:1]) * carry + other_ref[b, 1:2]
        start_ref[b] = jnp.where(core == 0, carry, passed)

    @pl.loop(0, batch)
    def _(b):
        carry = start_ref[b]
        for j in range(length // CHUNK):
            at = slice(j * CHUNK, (j + 1) * CHUNK)
            kept = carry * jnp.exp(-chunk_ref[b, j, 0:1])
            carry = kept + chunk_ref[b, j, 1:2]
            lanes = jnp.zeros((CHUNK, 128), jnp.float32)
            for k in range(width // 128):
                cols = slice(k * 128, (k + 1) * 128)
                gated = (run_ref[b, at, cols] + kept[:, cols]) * open_ref[b, at, cols]
                gated_ref[b, at, cols] = gated
                lanes = lanes + gated * gated
            power_ref[b, j] = jnp.sum(lanes.T, axis=0, keepdims=True)


def norm_kernel(channels, eps, gated_ref, power_ref, gain_ref, out_hbm, out_ref, sems):
    batch, length, width = gated_ref.shape
    chunks = length // CHUNK

    def store(b, j):
        at = pl.ds(j * CHUNK, CHUNK)
        return pltpu.make_async_copy(out_ref.at[b, at], out_hbm.at[b, at], sems.at[b, j])

    @pl.loop(0, batch)
    def _(b):
        for j in range(chunks):
            at = slice(j * CHUNK, (j + 1) * CHUNK)
            rate = lax.rsqrt(power_ref[b, j] * (1.0 / channels) + eps)
            rate = jnp.broadcast_to(rate, (128, CHUNK)).T
            for k in range(width // 128):
                cols = slice(k * 128, (k + 1) * 128)
                out = gated_ref[b, at, cols] * rate * gain_ref[:, cols]
                out_ref[b, at, cols] = out.astype(jnp.bfloat16)
            store(b, j).start()

    for b in range(batch):
        for j in range(chunks):
            store(b, j).wait()


def params(mib):
    return pltpu.CompilerParams(vmem_limit_bytes=mib * 1024 * 1024)


def total_over_chan(x):
    x = x + lax.ppermute(x, "chan", [(i, i ^ 1) for i in range(4)])
    return x + lax.ppermute(x, "chan", [(i, i ^ 3) for i in range(4)])


def body(decay_rate, drive_in, gate_in, norm_gain):
    batch, length, width = decay_rate.shape
    total_length = length * lax.axis_size(TIME)
    channels = width * lax.axis_size("chan")
    chunks = length // CHUNK
    f32 = jnp.float32
    shape = (batch, length, width)
    hbm = pl.BlockSpec(memory_space=pltpu.HBM)
    vmem = pl.BlockSpec(memory_space=pltpu.VMEM)

    place = lax.axis_index(TIME).astype(jnp.int32).reshape(1)
    smem = pl.BlockSpec(memory_space=pltpu.SMEM)

    chunk, total, run, logs, gate = pl.pallas_call(
        lambda *refs: local_kernel(1.0 / total_length, *refs),
        in_specs=[smem, hbm, hbm, hbm],
        out_specs=[vmem] * 5,
        out_shape=[
            jax.ShapeDtypeStruct((batch, chunks, 2, width), f32),
            jax.ShapeDtypeStruct((batch, 2, width), f32),
            jax.ShapeDtypeStruct(shape, f32),
            jax.ShapeDtypeStruct(shape, f32),
            jax.ShapeDtypeStruct(shape, jnp.bfloat16),
        ],
        scratch_shapes=[
            pltpu.VMEM(shape, f32),
            pltpu.VMEM(shape, jnp.bfloat16),
            pltpu.VMEM((CHUNK, CHUNK), jnp.bfloat16),
            pltpu.VMEM((CHUNK, 2 * CHUNK), jnp.bfloat16),
            pltpu.SemaphoreType.DMA((2, batch, chunks)),
            pltpu.SemaphoreType.DMA,
        ],
        compiler_params=params(VMEM_LOCAL),
        name="local",
    )(place, *(pltpu.with_memory_space_constraint(x, pltpu.HBM) for x in (decay_rate, drive_in, gate_in)))

    peers = lax.axis_size(CHIPS)
    other = lax.ppermute(total, CORE, SWAP)
    small = pl.CostEstimate(flops=1_000_000_000, transcendentals=0, bytes_accessed=0)
    twice = pl.pallas_call(
        gate_kernel,
        in_specs=[vmem],
        out_specs=vmem,
        out_shape=jax.ShapeDtypeStruct(shape, f32),
        compiler_params=params(4),
        cost_estimate=small,
        name="gate",
    )(gate)
    sent = pl.pallas_call(
        pack_kernel,
        in_specs=[smem, vmem, vmem, pl.BlockSpec(memory_space=pl.ANY)],
        out_specs=vmem,
        out_shape=jax.ShapeDtypeStruct((peers, 2, batch // 2, width), f32),
        compiler_params=params(4),
        name="pack",
    )(place, total, other, twice)
    pieces = lax.all_to_all(sent, CHIPS, 0, 0)
    carry = pl.pallas_call(
        carry_kernel,
        in_specs=[smem, vmem],
        out_specs=vmem,
        out_shape=jax.ShapeDtypeStruct((batch // 2, width), f32),
        compiler_params=params(4),
        name="carry",
    )(place, pieces)
    across = lax.ppermute(carry, CORE, SWAP)
    opened = pl.pallas_call(
        open_kernel,
        in_specs=[vmem] * 3,
        out_specs=vmem,
        out_shape=jax.ShapeDtypeStruct(shape, f32),
        compiler_params=params(4),
        cost_estimate=small,
        name="open",
    )(carry, logs, twice)

    gated, power = pl.pallas_call(
        power_kernel,
        in_specs=[smem] + [vmem] * 6,
        out_specs=[vmem] * 2,
        out_shape=[
            jax.ShapeDtypeStruct(shape, f32),
            jax.ShapeDtypeStruct((batch, chunks, 1, CHUNK), f32),
        ],
        scratch_shapes=[pltpu.VMEM((batch, 1, width), f32)],
        compiler_params=params(VMEM_POWER),
        name="power",
    )(place, run, opened, chunk, carry, across, other)

    power = total_over_chan(power)

    return pl.pallas_call(
        lambda *refs: norm_kernel(channels, 4e-6 * total_length, *refs),
        in_specs=[vmem] * 3,
        out_specs=hbm,
        out_shape=jax.ShapeDtypeStruct(shape, jnp.bfloat16),
        scratch_shapes=[pltpu.VMEM(shape, jnp.bfloat16), pltpu.SemaphoreType.DMA((batch, chunks))],
        compiler_params=params(VMEM_NORM),
        name="norm",
    )(gated, power, norm_gain[None])


def solution(mesh):
    split = Mesh(
        mesh.devices.reshape(2, 4, 4, 2, mesh.shape["chan"]),
        TIME + ("chan",),
    )
    in_specs = (P(None, TIME, "chan"), P(None, TIME, "chan"), P(None, TIME, "chan"), P("chan"))
    out_specs = P(None, TIME, "chan")
    return jax.shard_map(body, mesh=split, in_specs=in_specs, out_specs=out_specs, check_vma=False)
```

```python
import jax
import jax.numpy as jnp
from jax import lax
from jax.experimental import pallas as pl
from jax.experimental.pallas import tpu as pltpu
from jax.sharding import Mesh
from jax.sharding import PartitionSpec as P

TIME = ("time_0", "time_1", "time_2", "time_3")
CHIPS = ("time_0", "time_1", "time_2")
CORE = "time_3"
CHUNK = 128
LOG2E = 1.4426950408889634
SWAP = [(0, 1), (1, 0)]
VMEM_LOCAL, VMEM_POWER, VMEM_NORM = 24, 8, 8


def columns(width):
    return [slice(k, min(k + 256, width)) for k in range(0, width, 256)]


def local_kernel(
    scale, place_ref, decay_hbm, drive_hbm, gate_hbm, chunk_ref, total_ref, run_ref, logs_ref,
    gate_ref, decay_ref, drive_ref, later_ref, upto_ref, sems, gate_sem,
):
    del place_ref
    batch, length, width = decay_ref.shape
    chunks = length // CHUNK

    def loads(b, j):
        at = pl.ds(j * CHUNK, CHUNK)
        pairs = ((decay_hbm, decay_ref), (drive_hbm, drive_ref))
        return [
            pltpu.make_async_copy(hbm.at[b, at], ref.at[b, at], sems.at[k, b, j])
            for k, (hbm, ref) in enumerate(pairs)
        ]

    for j in range(chunks):
        for copy in loads(0, j):
            copy.start()

    row = lax.broadcasted_iota(jnp.int32, (CHUNK, CHUNK), 0)
    col = lax.broadcasted_iota(jnp.int32, (CHUNK, CHUNK), 1)
    bf16, f32 = jnp.bfloat16, jnp.float32
    later_ref[...] = jnp.where(col > row, -scale, 0.0).astype(bf16)
    upto = jnp.where(col > row, 0.0, 1.0).astype(bf16)
    upto_ref[:, :CHUNK] = upto
    upto_ref[:, CHUNK:] = upto

    def chunk(b, j):
        at = slice(j * CHUNK, (j + 1) * CHUNK)
        for cols in columns(width):
            decay = decay_ref[b, at, cols]
            drive = drive_ref[b, at, cols]
            logs = jnp.dot(later_ref[...], decay.astype(bf16), preferred_element_type=f32)
            less = (jnp.exp2(logs * LOG2E) - 1.0).astype(bf16) * drive
            run = jnp.dot(
                upto_ref[...], jnp.concatenate([drive, less]), preferred_element_type=f32
            )
            run_ref[b, at, cols] = run
            logs_ref[b, at, cols] = logs
            pushed = run[CHUNK - 1 :]
            lost = jnp.sum(decay, axis=0, keepdims=True) * scale
            chunk_ref[b, j, 0:1, cols] = lost
            chunk_ref[b, j, 1:2, cols] = pushed
            if j == 0:
                total_ref[b, 0:1, cols] = lost
                total_ref[b, 1:2, cols] = pushed
            else:
                total_ref[b, 0:1, cols] = total_ref[b, 0:1, cols] + lost
                total_ref[b, 1:2, cols] = jnp.exp(-lost) * total_ref[b, 1:2, cols] + pushed

    gates = pltpu.make_async_copy(gate_hbm, gate_ref, gate_sem)
    for j in range(chunks):
        for copy in loads(1, j):
            copy.start()
    for j in range(chunks):
        for copy in loads(0, j):
            copy.wait()
        for copy in loads(2, j):
            copy.start()
        chunk(0, j)

    @pl.loop(1, batch)
    def _(b):
        for j in range(chunks):
            for copy in loads(b, j):
                copy.wait()

        @pl.when(b < batch - 2)
        def _():
            for j in range(chunks):
                for copy in loads(b + 2, j):
                    copy.start()

        @pl.when(b == 1)
        def _():
            gates.start()

        for j in range(chunks):
            chunk(b, j)

    gates.wait()


def gate_kernel(gate_ref, twice_ref):
    batch, length, width = gate_ref.shape

    @pl.loop(0, batch)
    def _(b):
        for j in range(length // CHUNK):
            at = slice(j * CHUNK, (j + 1) * CHUNK)
            for cols in columns(width):
                half = (gate_ref[b, at, cols] * jnp.bfloat16(0.5)).astype(jnp.float32)
                twice_ref[b, at, cols] = jnp.tanh(half) + 1.0


def open_kernel(after_ref, logs_ref, twice_ref, open_ref):
    del after_ref
    batch, length, width = logs_ref.shape

    @pl.loop(0, batch)
    def _(b):
        for j in range(length // CHUNK):
            at = slice(j * CHUNK, (j + 1) * CHUNK)
            for cols in columns(width):
                lift = jnp.exp2(logs_ref[b, at, cols] * -LOG2E)
                open_ref[b, at, cols] = lift * twice_ref[b, at, cols]


def pack_kernel(place_ref, total_ref, other_ref, after_ref, sent_ref):
    del after_ref
    core = place_ref[0] % 2
    batch = total_ref.shape[0]

    def half(begin, first_ref, second_ref):
        for b in range(batch // 2):
            at = begin + b
            lost = second_ref[at, 0:1]
            pushed = jnp.exp(-lost) * first_ref[at, 1:2] + second_ref[at, 1:2]
            lost = lost + first_ref[at, 0:1]
            for k in range(sent_ref.shape[0]):
                sent_ref[k, 0, b : b + 1] = lost
                sent_ref[k, 1, b : b + 1] = pushed

    @pl.when(core == 0)
    def _():
        half(0, total_ref, other_ref)

    @pl.when(core == 1)
    def _():
        half(batch // 2, other_ref, total_ref)


def carry_kernel(place_ref, pieces_ref, carry_ref):
    chip = place_ref[0] // 2
    carry = jnp.zeros(carry_ref.shape, jnp.float32)
    for k in range(pieces_ref.shape[0] - 1):
        passed = jnp.exp(-pieces_ref[k, 0]) * carry + pieces_ref[k, 1]
        carry = jnp.where(k < chip, passed, carry)
    carry_ref[...] = carry


def power_kernel(own, place_ref, run_ref, open_ref, chunk_ref, carry_ref, other_ref, *refs):
    gated_ref, power_ref = refs[-2:]
    batch, length, width = run_ref.shape
    core = place_ref[0] % 2
    begin = (core if own else 1 - core) * (batch // 2)
    for i in range(batch // 2):
        b = begin + i
        carry = carry_ref[i : i + 1]
        passed = jnp.exp(-other_ref[b, 0:1]) * carry + other_ref[b, 1:2]
        carry = jnp.where(core == 0, carry, passed)
        for j in range(length // CHUNK):
            at = slice(j * CHUNK, (j + 1) * CHUNK)
            kept = carry * jnp.exp(-chunk_ref[b, j, 0:1])
            carry = kept + chunk_ref[b, j, 1:2]
            lanes = jnp.zeros((CHUNK, 128), jnp.float32)
            for k in range(width // 128):
                cols = slice(k * 128, (k + 1) * 128)
                gated = (run_ref[b, at, cols] + kept[:, cols]) * open_ref[b, at, cols]
                gated_ref[b, at, cols] = gated
                lanes = lanes + gated * gated
            power_ref[b, j] = jnp.sum(lanes.T, axis=0, keepdims=True)


def norm_kernel(channels, eps, gated_ref, power_ref, gain_ref, out_hbm, out_ref, sems):
    batch, length, width = gated_ref.shape
    chunks = length // CHUNK

    def store(b, j):
        at = pl.ds(j * CHUNK, CHUNK)
        return pltpu.make_async_copy(out_ref.at[b, at], out_hbm.at[b, at], sems.at[b, j])

    @pl.loop(0, batch)
    def _(b):
        for j in range(chunks):
            at = slice(j * CHUNK, (j + 1) * CHUNK)
            rate = lax.rsqrt(power_ref[b, j] * (1.0 / channels) + eps)
            rate = jnp.broadcast_to(rate, (128, CHUNK)).T
            for k in range(width // 128):
                cols = slice(k * 128, (k + 1) * 128)
                out = gated_ref[b, at, cols] * rate * gain_ref[:, cols]
                out_ref[b, at, cols] = out.astype(jnp.bfloat16)
            store(b, j).start()

    for b in range(batch):
        for j in range(chunks):
            store(b, j).wait()


def params(mib):
    return pltpu.CompilerParams(vmem_limit_bytes=mib * 1024 * 1024)


def total_over_chan(x):
    x = x + lax.ppermute(x, "chan", [(i, i ^ 1) for i in range(4)])
    return x + lax.ppermute(x, "chan", [(i, i ^ 3) for i in range(4)])


def body(decay_rate, drive_in, gate_in, norm_gain):
    batch, length, width = decay_rate.shape
    total_length = length * lax.axis_size(TIME)
    channels = width * lax.axis_size("chan")
    chunks = length // CHUNK
    f32 = jnp.float32
    shape = (batch, length, width)
    hbm = pl.BlockSpec(memory_space=pltpu.HBM)
    vmem = pl.BlockSpec(memory_space=pltpu.VMEM)

    place = lax.axis_index(TIME).astype(jnp.int32).reshape(1)
    smem = pl.BlockSpec(memory_space=pltpu.SMEM)

    chunk, total, run, logs, gate = pl.pallas_call(
        lambda *refs: local_kernel(1.0 / total_length, *refs),
        in_specs=[smem, hbm, hbm, hbm],
        out_specs=[vmem] * 5,
        out_shape=[
            jax.ShapeDtypeStruct((batch, chunks, 2, width), f32),
            jax.ShapeDtypeStruct((batch, 2, width), f32),
            jax.ShapeDtypeStruct(shape, f32),
            jax.ShapeDtypeStruct(shape, f32),
            jax.ShapeDtypeStruct(shape, jnp.bfloat16),
        ],
        scratch_shapes=[
            pltpu.VMEM(shape, f32),
            pltpu.VMEM(shape, jnp.bfloat16),
            pltpu.VMEM((CHUNK, CHUNK), jnp.bfloat16),
            pltpu.VMEM((CHUNK, 2 * CHUNK), jnp.bfloat16),
            pltpu.SemaphoreType.DMA((2, batch, chunks)),
            pltpu.SemaphoreType.DMA,
        ],
        compiler_params=params(VMEM_LOCAL),
        name="local",
    )(place, *(pltpu.with_memory_space_constraint(x, pltpu.HBM) for x in (decay_rate, drive_in, gate_in)))

    peers = lax.axis_size(CHIPS)
    other = lax.ppermute(total, CORE, SWAP)
    small = pl.CostEstimate(flops=1_000_000_000, transcendentals=0, bytes_accessed=0)
    twice = pl.pallas_call(
        gate_kernel,
        in_specs=[vmem],
        out_specs=vmem,
        out_shape=jax.ShapeDtypeStruct(shape, f32),
        compiler_params=params(4),
        cost_estimate=small,
        name="gate",
    )(gate)
    sent = pl.pallas_call(
        pack_kernel,
        in_specs=[smem, vmem, vmem, pl.BlockSpec(memory_space=pl.ANY)],
        out_specs=vmem,
        out_shape=jax.ShapeDtypeStruct((peers, 2, batch // 2, width), f32),
        compiler_params=params(4),
        name="pack",
    )(place, total, other, twice)
    pieces = lax.all_to_all(sent, CHIPS, 0, 0)
    carry = pl.pallas_call(
        carry_kernel,
        in_specs=[smem, vmem],
        out_specs=vmem,
        out_shape=jax.ShapeDtypeStruct((batch // 2, width), f32),
        compiler_params=params(4),
        name="carry",
    )(place, pieces)
    across = lax.ppermute(carry, CORE, SWAP)
    opened = pl.pallas_call(
        open_kernel,
        in_specs=[vmem] * 3,
        out_specs=vmem,
        out_shape=jax.ShapeDtypeStruct(shape, f32),
        compiler_params=params(4),
        cost_estimate=small,
        name="open",
    )(carry, logs, twice)

    def powers(own, carry, *before):
        return pl.pallas_call(
            lambda *refs: power_kernel(own, *refs),
            in_specs=[smem] + [vmem] * (5 + len(before)),
            out_specs=[vmem] * 2,
            out_shape=[
                jax.ShapeDtypeStruct(shape, f32),
                jax.ShapeDtypeStruct((batch, chunks, 1, CHUNK), f32),
            ],
            input_output_aliases={6 + k: k for k in range(len(before))},
            compiler_params=params(VMEM_POWER),
            name="own" if own else "rest",
        )(place, run, opened, chunk, carry, other, *before)

    gated, power = powers(False, across, *powers(True, carry))

    power = total_over_chan(power)

    return pl.pallas_call(
        lambda *refs: norm_kernel(channels, 4e-6 * total_length, *refs),
        in_specs=[vmem] * 3,
        out_specs=hbm,
        out_shape=jax.ShapeDtypeStruct(shape, jnp.bfloat16),
        scratch_shapes=[pltpu.VMEM(shape, jnp.bfloat16), pltpu.SemaphoreType.DMA((batch, chunks))],
        compiler_params=params(VMEM_NORM),
        name="norm",
    )(gated, power, norm_gain[None])


def solution(mesh):
    split = Mesh(
        mesh.devices.reshape(2, 4, 4, 2, mesh.shape["chan"]),
        TIME + ("chan",),
    )
    in_specs = (P(None, TIME, "chan"), P(None, TIME, "chan"), P(None, TIME, "chan"), P("chan"))
    out_specs = P(None, TIME, "chan")
    return jax.shard_map(body, mesh=split, in_specs=in_specs, out_specs=out_specs, check_vma=False)
```

```python
import jax
import jax.numpy as jnp
from jax import lax
from jax.experimental import pallas as pl
from jax.experimental.pallas import tpu as pltpu
from jax.sharding import Mesh
from jax.sharding import PartitionSpec as P

TIME = ("time_0", "time_1", "time_2", "time_3")
CHIPS = ("time_0", "time_1", "time_2")
CORE = "time_3"
CHUNK = 128
LOG2E = 1.4426950408889634
SWAP = [(0, 1), (1, 0)]
VMEM_LOCAL, VMEM_POWER, VMEM_NORM = 24, 8, 8


def columns(width):
    return [slice(k, min(k + 256, width)) for k in range(0, width, 256)]


def local_kernel(
    scale, place_ref, decay_hbm, drive_hbm, gate_hbm, chunk_ref, total_ref, run_ref, logs_ref,
    gate_ref, decay_ref, drive_ref, later_ref, upto_ref, sems, gate_sem,
):
    del place_ref
    batch, length, width = decay_ref.shape
    chunks = length // CHUNK

    def loads(b, j):
        at = pl.ds(j * CHUNK, CHUNK)
        pairs = ((decay_hbm, decay_ref), (drive_hbm, drive_ref))
        return [
            pltpu.make_async_copy(hbm.at[b, at], ref.at[b, at], sems.at[k, b, j])
            for k, (hbm, ref) in enumerate(pairs)
        ]

    for j in range(chunks):
        for copy in loads(0, j):
            copy.start()

    row = lax.broadcasted_iota(jnp.int32, (CHUNK, CHUNK), 0)
    col = lax.broadcasted_iota(jnp.int32, (CHUNK, CHUNK), 1)
    bf16, f32 = jnp.bfloat16, jnp.float32
    later_ref[...] = jnp.where(col > row, -scale, 0.0).astype(bf16)
    upto = jnp.where(col > row, 0.0, 1.0).astype(bf16)
    upto_ref[:, :CHUNK] = upto
    upto_ref[:, CHUNK:] = upto

    def chunk(b, j):
        at = slice(j * CHUNK, (j + 1) * CHUNK)
        for cols in columns(width):
            decay = decay_ref[b, at, cols]
            drive = drive_ref[b, at, cols]
            logs = jnp.dot(later_ref[...], decay.astype(bf16), preferred_element_type=f32)
            less = (jnp.exp2(logs * LOG2E) - 1.0).astype(bf16) * drive
            run = jnp.dot(
                upto_ref[...], jnp.concatenate([drive, less]), preferred_element_type=f32
            )
            run_ref[b, at, cols] = run
            logs_ref[b, at, cols] = logs
            pushed = run[CHUNK - 1 :]
            lost = jnp.sum(decay, axis=0, keepdims=True) * scale
            chunk_ref[b, j, 0:1, cols] = lost
            chunk_ref[b, j, 1:2, cols] = pushed
            if j == 0:
                total_ref[b, 0:1, cols] = lost
                total_ref[b, 1:2, cols] = pushed
            else:
                total_ref[b, 0:1, cols] = total_ref[b, 0:1, cols] + lost
                total_ref[b, 1:2, cols] = jnp.exp(-lost) * total_ref[b, 1:2, cols] + pushed

    gates = pltpu.make_async_copy(gate_hbm, gate_ref, gate_sem)
    def whole(b):
        pairs = ((decay_hbm, decay_ref), (drive_hbm, drive_ref))
        return [
            pltpu.make_async_copy(hbm.at[b], ref.at[b], sems.at[k, b, 0])
            for k, (hbm, ref) in enumerate(pairs)
        ]

    for b in (1, 2):
        for copy in whole(b):
            copy.start()
    for j in range(chunks):
        for copy in loads(0, j):
            copy.wait()
        if j == 0:
            for copy in whole(3):
                copy.start()
            gates.start()
        chunk(0, j)

    @pl.loop(1, batch)
    def _(b):
        for copy in whole(b):
            copy.wait()
        for j in range(chunks):
            chunk(b, j)

    gates.wait()


def gate_kernel(gate_ref, twice_ref):
    batch, length, width = gate_ref.shape

    @pl.loop(0, batch)
    def _(b):
        for j in range(length // CHUNK):
            at = slice(j * CHUNK, (j + 1) * CHUNK)
            for cols in columns(width):
                half = (gate_ref[b, at, cols] * jnp.bfloat16(0.5)).astype(jnp.float32)
                twice_ref[b, at, cols] = jnp.tanh(half) + 1.0


def open_kernel(after_ref, logs_ref, twice_ref, open_ref):
    del after_ref
    batch, length, width = logs_ref.shape

    @pl.loop(0, batch)
    def _(b):
        for j in range(length // CHUNK):
            at = slice(j * CHUNK, (j + 1) * CHUNK)
            for cols in columns(width):
                lift = jnp.exp2(logs_ref[b, at, cols] * -LOG2E)
                open_ref[b, at, cols] = lift * twice_ref[b, at, cols]


def pack_kernel(place_ref, total_ref, other_ref, after_ref, sent_ref):
    del after_ref
    core = place_ref[0] % 2
    batch = total_ref.shape[0]

    def half(begin, first_ref, second_ref):
        for b in range(batch // 2):
            at = begin + b
            lost = second_ref[at, 0:1]
            pushed = jnp.exp(-lost) * first_ref[at, 1:2] + second_ref[at, 1:2]
            lost = lost + first_ref[at, 0:1]
            for k in range(sent_ref.shape[0]):
                sent_ref[k, 0, b : b + 1] = lost
                sent_ref[k, 1, b : b + 1] = pushed

    @pl.when(core == 0)
    def _():
        half(0, total_ref, other_ref)

    @pl.when(core == 1)
    def _():
        half(batch // 2, other_ref, total_ref)


def carry_kernel(place_ref, pieces_ref, carry_ref):
    chip = place_ref[0] // 2
    carry = jnp.zeros(carry_ref.shape, jnp.float32)
    for k in range(pieces_ref.shape[0] - 1):
        passed = jnp.exp(-pieces_ref[k, 0]) * carry + pieces_ref[k, 1]
        carry = jnp.where(k < chip, passed, carry)
    carry_ref[...] = carry


def power_kernel(own, place_ref, run_ref, open_ref, chunk_ref, carry_ref, other_ref, *refs):
    gated_ref, power_ref = refs[-2:]
    batch, length, width = run_ref.shape
    core = place_ref[0] % 2
    begin = (core if own else 1 - core) * (batch // 2)
    for i in range(batch // 2):
        b = begin + i
        carry = carry_ref[i : i + 1]
        passed = jnp.exp(-other_ref[b, 0:1]) * carry + other_ref[b, 1:2]
        carry = jnp.where(core == 0, carry, passed)
        for j in range(length // CHUNK):
            at = slice(j * CHUNK, (j + 1) * CHUNK)
            kept = carry * jnp.exp(-chunk_ref[b, j, 0:1])
            carry = kept + chunk_ref[b, j, 1:2]
            lanes = jnp.zeros((CHUNK, 128), jnp.float32)
            for k in range(width // 128):
                cols = slice(k * 128, (k + 1) * 128)
                gated = (run_ref[b, at, cols] + kept[:, cols]) * open_ref[b, at, cols]
                gated_ref[b, at, cols] = gated
                lanes = lanes + gated * gated
            power_ref[b, j] = jnp.sum(lanes.T, axis=0, keepdims=True)


def norm_kernel(channels, eps, gated_ref, power_ref, gain_ref, out_hbm, out_ref, sems):
    batch, length, width = gated_ref.shape
    chunks = length // CHUNK

    def store(b, j):
        at = pl.ds(j * CHUNK, CHUNK)
        return pltpu.make_async_copy(out_ref.at[b, at], out_hbm.at[b, at], sems.at[b, j])

    @pl.loop(0, batch)
    def _(b):
        for j in range(chunks):
            at = slice(j * CHUNK, (j + 1) * CHUNK)
            rate = lax.rsqrt(power_ref[b, j] * (1.0 / channels) + eps)
            rate = jnp.broadcast_to(rate, (128, CHUNK)).T
            for k in range(width // 128):
                cols = slice(k * 128, (k + 1) * 128)
                out = gated_ref[b, at, cols] * rate * gain_ref[:, cols]
                out_ref[b, at, cols] = out.astype(jnp.bfloat16)
            store(b, j).start()

    for b in range(batch):
        for j in range(chunks):
            store(b, j).wait()


def params(mib):
    return pltpu.CompilerParams(vmem_limit_bytes=mib * 1024 * 1024)


def total_over_chan(x):
    x = x + lax.ppermute(x, "chan", [(i, i ^ 1) for i in range(4)])
    return x + lax.ppermute(x, "chan", [(i, i ^ 3) for i in range(4)])


def body(decay_rate, drive_in, gate_in, norm_gain):
    batch, length, width = decay_rate.shape
    total_length = length * lax.axis_size(TIME)
    channels = width * lax.axis_size("chan")
    chunks = length // CHUNK
    f32 = jnp.float32
    shape = (batch, length, width)
    hbm = pl.BlockSpec(memory_space=pltpu.HBM)
    vmem = pl.BlockSpec(memory_space=pltpu.VMEM)

    place = lax.axis_index(TIME).astype(jnp.int32).reshape(1)
    smem = pl.BlockSpec(memory_space=pltpu.SMEM)

    chunk, total, run, logs, gate = pl.pallas_call(
        lambda *refs: local_kernel(1.0 / total_length, *refs),
        in_specs=[smem, hbm, hbm, hbm],
        out_specs=[vmem] * 5,
        out_shape=[
            jax.ShapeDtypeStruct((batch, chunks, 2, width), f32),
            jax.ShapeDtypeStruct((batch, 2, width), f32),
            jax.ShapeDtypeStruct(shape, f32),
            jax.ShapeDtypeStruct(shape, f32),
            jax.ShapeDtypeStruct(shape, jnp.bfloat16),
        ],
        scratch_shapes=[
            pltpu.VMEM(shape, f32),
            pltpu.VMEM(shape, jnp.bfloat16),
            pltpu.VMEM((CHUNK, CHUNK), jnp.bfloat16),
            pltpu.VMEM((CHUNK, 2 * CHUNK), jnp.bfloat16),
            pltpu.SemaphoreType.DMA((2, batch, chunks)),
            pltpu.SemaphoreType.DMA,
        ],
        compiler_params=params(VMEM_LOCAL),
        name="local",
    )(place, *(pltpu.with_memory_space_constraint(x, pltpu.HBM) for x in (decay_rate, drive_in, gate_in)))

    peers = lax.axis_size(CHIPS)
    other = lax.ppermute(total, CORE, SWAP)
    small = pl.CostEstimate(flops=1_000_000_000, transcendentals=0, bytes_accessed=0)
    twice = pl.pallas_call(
        gate_kernel,
        in_specs=[vmem],
        out_specs=vmem,
        out_shape=jax.ShapeDtypeStruct(shape, f32),
        compiler_params=params(4),
        cost_estimate=small,
        name="gate",
    )(gate)
    sent = pl.pallas_call(
        pack_kernel,
        in_specs=[smem, vmem, vmem, pl.BlockSpec(memory_space=pl.ANY)],
        out_specs=vmem,
        out_shape=jax.ShapeDtypeStruct((peers, 2, batch // 2, width), f32),
        compiler_params=params(4),
        name="pack",
    )(place, total, other, twice)
    pieces = lax.all_to_all(sent, CHIPS, 0, 0)
    carry = pl.pallas_call(
        carry_kernel,
        in_specs=[smem, vmem],
        out_specs=vmem,
        out_shape=jax.ShapeDtypeStruct((batch // 2, width), f32),
        compiler_params=params(4),
        name="carry",
    )(place, pieces)
    across = lax.ppermute(carry, CORE, SWAP)
    opened = pl.pallas_call(
        open_kernel,
        in_specs=[vmem] * 3,
        out_specs=vmem,
        out_shape=jax.ShapeDtypeStruct(shape, f32),
        compiler_params=params(4),
        cost_estimate=small,
        name="open",
    )(carry, logs, twice)

    def powers(own, carry, *before):
        return pl.pallas_call(
            lambda *refs: power_kernel(own, *refs),
            in_specs=[smem] + [vmem] * (5 + len(before)),
            out_specs=[vmem] * 2,
            out_shape=[
                jax.ShapeDtypeStruct(shape, f32),
                jax.ShapeDtypeStruct((batch, chunks, 1, CHUNK), f32),
            ],
            input_output_aliases={6 + k: k for k in range(len(before))},
            compiler_params=params(VMEM_POWER),
            name="own" if own else "rest",
        )(place, run, opened, chunk, carry, other, *before)

    gated, power = powers(False, across, *powers(True, carry))

    power = total_over_chan(power)

    return pl.pallas_call(
        lambda *refs: norm_kernel(channels, 4e-6 * total_length, *refs),
        in_specs=[vmem] * 3,
        out_specs=hbm,
        out_shape=jax.ShapeDtypeStruct(shape, jnp.bfloat16),
        scratch_shapes=[pltpu.VMEM(shape, jnp.bfloat16), pltpu.SemaphoreType.DMA((batch, chunks))],
        compiler_params=params(VMEM_NORM),
        name="norm",
    )(gated, power, norm_gain[None])


def solution(mesh):
    split = Mesh(
        mesh.devices.reshape(2, 4, 4, 2, mesh.shape["chan"]),
        TIME + ("chan",),
    )
    in_specs = (P(None, TIME, "chan"), P(None, TIME, "chan"), P(None, TIME, "chan"), P("chan"))
    out_specs = P(None, TIME, "chan")
    return jax.shard_map(body, mesh=split, in_specs=in_specs, out_specs=out_specs, check_vma=False)
```
